16 devices in a mesh: data: 4 (over z, y), stage: 4 (over x, core).
Axes of the slice: x: 2, y: 2, z: 2, core: 2. Of those that a mesh axis runs over, the one named last changes fastest.
Arguments:
- w_first: float32 [4, 128, 512], P('stage')
- w_second: float32 [4, 512, 128], P('stage')
- mom_first: float32 [4, 128, 512], P('stage')
- mom_second: float32 [4, 512, 128], P('stage')
- vel_first: float32 [4, 128, 512], P('stage')
- vel_second: float32 [4, 512, 128], P('stage')
- grad_first: float32 [4, 128, 512], P('stage')
- grad_second: float32 [4, 512, 128], P('stage')
- embed_table: float32 [30528, 128], replicated
- mom_embed: float32 [30528, 128], replicated
- vel_embed: float32 [30528, 128], replicated
- grad_embed: float32 [30528, 128], replicated
- stage_acts: bfloat16 [4, 4096, 128], P('stage', 'data')
- last_tokens: int32 [4096], P('data')
- targets: int32 [4096], P('data')
- next_tokens: int32 [16, 4096], P(None, 'data')
- max_norm: float32 [1], replicated
Outputs:
- output 1: float32 [4, 128, 512], P('stage')
- output 2: float32 [4, 512, 128], P('stage')
- output 3: float32 [4, 128, 512], P('stage')
- output 4: float32 [4, 512, 128], P('stage')
- output 5: float32 [4, 128, 512], P('stage')
- output 6: float32 [4, 512, 128], P('stage')
- output 7: float32 [30528, 128], replicated
- output 8: float32 [30528, 128], replicated
- output 9: float32 [30528, 128], replicated
- output 10: bfloat16 [16, 4096, 128], P(None, 'data')
All inputs are finite; a program needn't handle non-finite values.
Results may differ from the reference program's by a relative error of at most 0.00627237.
Values are sent between devices in bfloat16 or wider.
A program may use at most 1 GiB of HBM per device.

```python
import jax
import jax.numpy as jnp
from jax import lax

D = 128
FF = 512
VOCAB = 30528
TOKENS = 1024
NEXT_MICRO = 16
STAGES = 4
REPLICAS = 4
STEP_COUNT = 10

EMB_SCALE = D ** 0.5
LEARN_RATE = 1e-3
ADAM_BETA1 = 0.9
ADAM_BETA2 = 0.95
ADAM_EPS = 1e-8
WEIGHT_DECAY = 0.1
CLIP_EPS = 1e-6


def setup_inputs(seed: int = 0) -> dict:
    rng_keys = jax.random.split(jax.random.key(seed), 17)
    n_rows = REPLICAS * TOKENS
    scale_first = 0.5 * (TOKENS / (FF * STAGES * REPLICAS)) ** 0.5
    scale_second = 0.5 * (TOKENS / (D * REPLICAS)) ** 0.5
    scale_embed = (TOKENS / (VOCAB * REPLICAS)) ** 0.5
    shape_first = (STAGES, D, FF)
    shape_second = (STAGES, FF, D)
    shape_embed = (VOCAB, D)
    w_first = jax.random.normal(rng_keys[0], shape_first, jnp.float32) * D ** -0.5
    w_second = jax.random.normal(rng_keys[1], shape_second, jnp.float32) * (FF * STAGES) ** -0.5
    embed_table = jax.random.normal(rng_keys[2], shape_embed, jnp.float32) * D ** -0.5
    grad_first = jax.random.normal(rng_keys[3], shape_first, jnp.float32) * scale_first
    grad_second = jax.random.normal(rng_keys[4], shape_second, jnp.float32) * scale_second
    grad_embed = jax.random.normal(rng_keys[5], shape_embed, jnp.float32) * scale_embed
    mom_first = jax.random.normal(rng_keys[6], shape_first, jnp.float32) * (0.4 * scale_first)
    mom_second = jax.random.normal(rng_keys[7], shape_second, jnp.float32) * (0.4 * scale_second)
    mom_embed = jax.random.normal(rng_keys[8], shape_embed, jnp.float32) * (0.4 * scale_embed)
    vel_first = jax.random.uniform(rng_keys[9], shape_first, jnp.float32, 0.25, 1.25) * (0.4 * scale_first) ** 2
    vel_second = jax.random.uniform(rng_keys[10], shape_second, jnp.float32, 0.25, 1.25) * (0.4 * scale_second) ** 2
    vel_embed = jax.random.uniform(rng_keys[11], shape_embed, jnp.float32, 0.25, 1.25) * (0.4 * scale_embed) ** 2
    stage_acts = jax.random.normal(rng_keys[12], (STAGES, n_rows, D), jnp.float32).astype(jnp.bfloat16)
    last_tokens = jax.random.randint(rng_keys[13], (n_rows,), 0, VOCAB, jnp.int32)
    targets = jax.random.randint(rng_keys[14], (n_rows,), 0, VOCAB, jnp.int32)
    next_tokens = jax.random.randint(rng_keys[15], (NEXT_MICRO, n_rows), 0, VOCAB, jnp.int32)
    grad_size = jnp.sqrt(jnp.sum(grad_first ** 2) + jnp.sum(grad_second ** 2) + jnp.sum(grad_embed ** 2))
    max_norm = grad_size * jax.random.uniform(rng_keys[16], (1,), jnp.float32, 0.5, 0.8)
    return {'w_first': w_first, 'w_second': w_second, 'mom_first': mom_first, 'mom_second': mom_second,
            'vel_first': vel_first, 'vel_second': vel_second, 'grad_first': grad_first, 'grad_second': grad_second,
            'embed_table': embed_table, 'mom_embed': mom_embed, 'vel_embed': vel_embed, 'grad_embed': grad_embed,
            'stage_acts': stage_acts, 'last_tokens': last_tokens, 'targets': targets, 'next_tokens': next_tokens,
            'max_norm': max_norm}


def block_forward(act_in, w_in, w_out):
    pre_act = jnp.dot(act_in, w_in, preferred_element_type=jnp.float32)
    hidden = jax.nn.gelu(pre_act).astype(jnp.bfloat16)
    mlp_out = jnp.dot(hidden, w_out, preferred_element_type=jnp.float32)
    return (act_in.astype(jnp.float32) + mlp_out).astype(jnp.bfloat16)


def block_backward(d_out, inputs):
    act_in, w_in, w_out = inputs
    pre_act = jnp.dot(act_in, w_in, preferred_element_type=jnp.float32)
    hidden, gelu_back = jax.vjp(jax.nn.gelu, pre_act)
    grad_out = jnp.dot(hidden.astype(jnp.bfloat16).T, d_out, preferred_element_type=jnp.float32)
    d_hidden = jnp.dot(d_out, w_out.T, preferred_element_type=jnp.float32)
    d_pre = gelu_back(d_hidden)[0].astype(jnp.bfloat16)
    grad_in = jnp.dot(act_in.T, d_pre, preferred_element_type=jnp.float32)
    d_act = (d_out.astype(jnp.float32) + jnp.dot(d_pre, w_in.T, preferred_element_type=jnp.float32)).astype(jnp.bfloat16)
    return d_act, (grad_in, grad_out)


def adamw_update(master, moment, velocity, gradient, clip_scale):
    scaled_grad = clip_scale * gradient
    moment_new = ADAM_BETA1 * moment + (1.0 - ADAM_BETA1) * scaled_grad
    velocity_new = ADAM_BETA2 * velocity + (1.0 - ADAM_BETA2) * scaled_grad * scaled_grad
    moment_hat = moment_new / (1.0 - ADAM_BETA1 ** STEP_COUNT)
    velocity_hat = velocity_new / (1.0 - ADAM_BETA2 ** STEP_COUNT)
    master_new = master - LEARN_RATE * (moment_hat / (jnp.sqrt(velocity_hat) + ADAM_EPS) + WEIGHT_DECAY * master)
    return master_new, moment_new, velocity_new


def reference(w_first, w_second, mom_first, mom_second, vel_first, vel_second, grad_first, grad_second,
              embed_table, mom_embed, vel_embed, grad_embed, stage_acts, last_tokens, targets, next_tokens, max_norm):
    first_b = w_first.astype(jnp.bfloat16)
    second_b = w_second.astype(jnp.bfloat16)
    table_b = embed_table.astype(jnp.bfloat16)
    vocab_ids = jnp.arange(VOCAB)

    def replica_step(grad_sums, inputs):
        acts_rep, tok_rep, tgt_rep = inputs
        top_out = block_forward(acts_rep[STAGES - 1], first_b[STAGES - 1], second_b[STAGES - 1])
        logits = jnp.dot(top_out, table_b.T, preferred_element_type=jnp.float32)
        soft_probs = jax.nn.softmax(logits, axis=-1)
        d_logits = jnp.where(vocab_ids[None, :] == tgt_rep[:, None], soft_probs - 1.0, soft_probs).astype(jnp.bfloat16)
        d_top = jnp.dot(d_logits, table_b, preferred_element_type=jnp.float32).astype(jnp.bfloat16)
        head_grad = jnp.dot(d_logits.T, top_out, preferred_element_type=jnp.float32)
        d_low, (grads_in, grads_out) = lax.scan(block_backward, d_top, (acts_rep, first_b, second_b), reverse=True)
        low_grad = EMB_SCALE * jax.ops.segment_sum(d_low.astype(jnp.float32), tok_rep, num_segments=VOCAB)
        sum_first, sum_second, sum_embed = grad_sums
        return (sum_first + grads_in, sum_second + grads_out, sum_embed + head_grad + low_grad), None

    per_replica = (jnp.transpose(stage_acts.reshape(STAGES, REPLICAS, TOKENS, D), (1, 0, 2, 3)),
                   last_tokens.reshape(REPLICAS, TOKENS), targets.reshape(REPLICAS, TOKENS))
    zero_init = (jnp.zeros_like(w_first), jnp.zeros_like(w_second), jnp.zeros_like(embed_table))
    (sum_first, sum_second, sum_embed), _ = lax.scan(replica_step, zero_init, per_replica)
    full_first = grad_first + sum_first / REPLICAS
    full_second = grad_second + sum_second / REPLICAS
    full_embed = grad_embed + sum_embed / REPLICAS
    total_sq = jnp.sum(full_first ** 2) + jnp.sum(full_second ** 2) + jnp.sum(full_embed ** 2)
    clip_scale = jnp.minimum(1.0, max_norm[0] / (jnp.sqrt(total_sq) + CLIP_EPS))
    new_first, new_mom_first, new_vel_first = adamw_update(w_first, mom_first, vel_first, full_first, clip_scale)
    new_second, new_mom_second, new_vel_second = adamw_update(w_second, mom_second, vel_second, full_second, clip_scale)
    new_embed, new_mom_embed, new_vel_embed = adamw_update(embed_table, mom_embed, vel_embed, full_embed, clip_scale)
    next_first_b = new_first.astype(jnp.bfloat16)
    next_second_b = new_second.astype(jnp.bfloat16)
    next_table_b = new_embed.astype(jnp.bfloat16)

    def run_rows(tok_row):
        start_act = (EMB_SCALE * jnp.take(next_table_b, tok_row, axis=0).astype(jnp.float32)).astype(jnp.bfloat16)

        def layer_step(carry_act, weights):
            return block_forward(carry_act, weights[0], weights[1]), None

        out_act, _ = lax.scan(layer_step, start_act, (next_first_b, next_second_b))
        return out_act

    next_acts = lax.map(run_rows, next_tokens.reshape(NEXT_MICRO * REPLICAS, TOKENS)).reshape(NEXT_MICRO, REPLICAS * TOKENS, D)
    return (new_first, new_second, new_mom_first, new_mom_second, new_vel_first, new_vel_second,
            new_embed, new_mom_embed, new_vel_embed, next_acts)
```

```python
import functools
import math
import jax
import jax.numpy as jnp
from jax import lax
from jax.experimental import pallas as pl
from jax.experimental.pallas import tpu as pltpu
from jax.sharding import PartitionSpec as P

STEP_COUNT = 10
LEARN_RATE = 1e-3
ADAM_BETA1 = 0.9
ADAM_BETA2 = 0.95
ADAM_EPS = 1e-8
WEIGHT_DECAY = 0.1
CLIP_EPS = 1e-6
GELU_A = math.sqrt(2.0 / math.pi)
GELU_B = 0.044715

MESH = pl.DeviceIdType.MESH
F32 = jnp.float32
BF16 = jnp.bfloat16
VOCAB = 30528
D = 128
FF = 512
TOK = 1024
CHUNK = 256
SHARD = 1920
N_SHARD = 16
N_DEV = 16
VPAD = SHARD * N_SHARD
ANY = pl.BlockSpec(memory_space=pl.ANY)
VMEM = pl.BlockSpec(memory_space=pltpu.VMEM)
SMEM = pl.BlockSpec(memory_space=pltpu.SMEM)


def dot(a, b):
    return jnp.dot(a, b, preferred_element_type=F32)


def dot_nt(a, b):
    return lax.dot_general(a, b, (((1,), (1,)), ((), ())), preferred_element_type=F32)


def dot_tn(a, b):
    return lax.dot_general(a, b, (((0,), (0,)), ((), ())), preferred_element_type=F32)


def gelu(x):
    return x * (0.5 * (1.0 + jnp.tanh(x * (GELU_A + (GELU_A * GELU_B) * (x * x)))))


def block_forward(act_in, w_in, w_out):
    hidden = gelu(dot(act_in, w_in)).astype(BF16)
    return (act_in.astype(F32) + dot(hidden, w_out)).astype(BF16)


def group_peer(group, me, shift, n):
    slot = lax.rem(me + shift, n)
    if group == 'all':
        return slot, {'data': slot // 4, 'stage': lax.rem(slot, 4)}
    return slot, {group: slot}


def group_me(group):
    if group == 'all':
        return lax.axis_index('data') * 4 + lax.axis_index('stage'), N_DEV
    return lax.axis_index(group), 4


def exchange_kernel(items, *refs):
    n_items = len(items)
    ins, outs = refs[:n_items], refs[n_items:2 * n_items]
    send_sem, recv_sem, local_sem = refs[2 * n_items:]
    groups = sorted({g for g, _ in items})
    if 'all' in groups:
        greet = ['all']
    else:
        greet = groups
    barrier = pltpu.get_barrier_semaphore()
    count = 0
    for g in greet:
        me, n = group_me(g)
        for k in range(1, n):
            _, dev = group_peer(g, me, k, n)
            pl.semaphore_signal(barrier, inc=1, device_id=dev, device_id_type=MESH)
            count += 1
    pl.semaphore_wait(barrier, count)
    copies = []
    base = 0
    for i, (g, mode) in enumerate(items):
        me, n = group_me(g)
        for k in range(1, n):
            slot, dev = group_peer(g, me, k, n)
            src = ins[i] if mode == 'gather' else ins[i].at[slot]
            cp = pltpu.make_async_remote_copy(
                src_ref=src, dst_ref=outs[i].at[me], send_sem=send_sem.at[base], recv_sem=recv_sem.at[base],
                device_id=dev, device_id_type=MESH)
            cp.start()
            copies.append((cp, i, k, base))
            base += 1
    locs = []
    for i, (g, mode) in enumerate(items):
        me, n = group_me(g)
        src = ins[i] if mode == 'gather' else ins[i].at[me]
        cp = pltpu.make_async_copy(src, outs[i].at[me], local_sem.at[i])
        cp.start()
        locs.append(cp)
    for cp, i, k, b in copies:
        cp.wait_send()
        g, mode = items[i]
        me, n = group_me(g)
        frm = lax.rem(me + n - k, n)
        _, dev = group_peer(g, me, n - k, n)
        src = ins[i] if mode == 'gather' else ins[i].at[frm]
        pltpu.make_async_remote_copy(
            src_ref=src, dst_ref=outs[i].at[frm], send_sem=send_sem.at[b], recv_sem=recv_sem.at[b],
            device_id=dev, device_id_type=MESH).wait_recv()
    for cp in locs:
        cp.wait()


def exchange(cid, *items):
    plan = tuple((g, m) for _, g, m in items)
    shapes, n_rem = [], 0
    for a, g, m in items:
        n = N_DEV if g == 'all' else 4
        chunk = a.shape if m == 'gather' else a.shape[1:]
        shapes.append(jax.ShapeDtypeStruct((n,) + tuple(chunk), a.dtype))
        n_rem += n - 1
    return pl.pallas_call(
        functools.partial(exchange_kernel, plan),
        out_shape=tuple(shapes),
        in_specs=[ANY] * len(items),
        out_specs=tuple([ANY] * len(items)),
        scratch_shapes=[pltpu.SemaphoreType.DMA((n_rem,)), pltpu.SemaphoreType.DMA((n_rem,)),
                        pltpu.SemaphoreType.DMA((len(items),))],
        compiler_params=pltpu.CompilerParams(collective_id=cid, has_side_effects=True),
        name=f'exchange_{cid}',
    )(*[a for a, _, _ in items])


def spread_kernel(z_ref, out_ref, send_sem, recv_sem, local_sem):
    stage = lax.axis_index('stage')
    barrier = pltpu.get_barrier_semaphore()
    for k in range(1, 4):
        pl.semaphore_signal(barrier, inc=1, device_id={'stage': lax.rem(stage + k, 4)}, device_id_type=MESH)
    pl.semaphore_wait(barrier, 3)

    @pl.when(stage == 3)
    def _():
        cps = []
        for p in range(3):
            cp = pltpu.make_async_remote_copy(
                src_ref=z_ref.at[p], dst_ref=out_ref, send_sem=send_sem.at[p], recv_sem=recv_sem,
                device_id={'stage': p}, device_id_type=MESH)
            cp.start()
            cps.append(cp)
        own = pltpu.make_async_copy(z_ref.at[3], out_ref, local_sem)
        own.start()
        own.wait()
        for cp in cps:
            cp.wait_send()

    @pl.when(stage != 3)
    def _():
        pltpu.make_async_remote_copy(
            src_ref=z_ref.at[0], dst_ref=out_ref, send_sem=send_sem.at[0], recv_sem=recv_sem,
            device_id={'stage': 3}, device_id_type=MESH).wait_recv()


def spread(cid, z):
    return pl.pallas_call(
        spread_kernel,
        out_shape=jax.ShapeDtypeStruct((CHUNK, D), BF16),
        in_specs=[ANY], out_specs=ANY,
        scratch_shapes=[pltpu.SemaphoreType.DMA((3,)), pltpu.SemaphoreType.DMA, pltpu.SemaphoreType.DMA],
        compiler_params=pltpu.CompilerParams(collective_id=cid, has_side_effects=True),
        name=f'spread_{cid}',
    )(z.reshape(4, CHUNK, D))


def swap_kernel(half_ref, out_ref, send_sem, recv_sem, local_sem):
    stage = lax.axis_index('stage')
    core = lax.rem(stage, 2)
    partner = stage + 1 - 2 * core
    barrier = pltpu.get_barrier_semaphore()
    pl.semaphore_signal(barrier, inc=1, device_id={'stage': partner}, device_id_type=MESH)
    pl.semaphore_wait(barrier, 1)
    cp = pltpu.make_async_remote_copy(
        src_ref=half_ref, dst_ref=out_ref.at[core], send_sem=send_sem, recv_sem=recv_sem,
        device_id={'stage': partner}, device_id_type=MESH)
    cp.start()
    own = pltpu.make_async_copy(half_ref, out_ref.at[core], local_sem)
    own.start()
    own.wait()
    cp.wait_send()
    pltpu.make_async_remote_copy(
        src_ref=half_ref, dst_ref=out_ref.at[1 - core], send_sem=send_sem, recv_sem=recv_sem,
        device_id={'stage': partner}, device_id_type=MESH).wait_recv()


def swap(cid, half):
    return pl.pallas_call(
        swap_kernel,
        out_shape=jax.ShapeDtypeStruct((2,) + half.shape, half.dtype),
        in_specs=[VMEM], out_specs=VMEM,
        scratch_shapes=[pltpu.SemaphoreType.DMA, pltpu.SemaphoreType.DMA, pltpu.SemaphoreType.DMA],
        compiler_params=pltpu.CompilerParams(collective_id=cid, has_side_effects=True),
        name=f'swap_{cid}',
    )(half)


def head1_kernel(z_ref, tgt_ref, e_ref, dz_ref, lse_ref, eb, ex, mt, run_m, run_s):
    t = pl.program_id(0)
    n = pl.num_programs(0)

    @pl.when(t == 0)
    def _():
        run_m[...] = jnp.full_like(run_m, -1e30)
        run_s[...] = jnp.zeros_like(run_s)

    row = lax.broadcasted_iota(jnp.int32, (SHARD, D), 0) + t * SHARD
    tile = jnp.where(row < VOCAB, e_ref[...], 0.0).astype(BF16)
    eb[t] = tile
    lane = lax.broadcasted_iota(jnp.int32, (1, 128), 1)

    def logits_part(j, carry):
        part = eb[t, pl.ds(j * 384, 384), :]
        logits = dot_nt(z_ref[...], part)
        old = run_m[...]
        new = old
        cols = []
        for c in range(3):
            ok = lane + (t * SHARD + j * 384 + c * 128) < VOCAB
            col = jnp.where(ok, logits[:, c * 128:(c + 1) * 128], -1e30)
            cols.append(col)
            new = jnp.maximum(new, col)
        total = run_s[...] * jnp.exp(old - new)
        for c in range(3):
            e = jnp.exp(cols[c] - new)
            total = total + e
            ex[t, :, pl.ds(pl.multiple_of(j * 384 + c * 128, 128), 128)] = e
        mt[t, j] = new
        run_m[...] = new
        run_s[...] = total
        return carry

    lax.fori_loop(0, 5, logits_part, 0)

    @pl.when(t == n - 1)
    def _():
        top = jnp.max(run_m[...], axis=1, keepdims=True)
        total = jnp.sum(run_s[...] * jnp.exp(run_m[...] - top), axis=1, keepdims=True)
        lse_ref[...] = jnp.broadcast_to(top + jnp.log(total), lse_ref.shape)
        inv = 1.0 / total
        run_m[...] = jnp.broadcast_to(top, run_m.shape)
        run_s[...] = jnp.broadcast_to(inv, run_s.shape)
        hit = tgt_ref[...] - lax.broadcasted_iota(jnp.int32, (CHUNK, 128), 1)

        def back_tile(i, acc):
            tt = i // 5
            j = i - tt * 5
            scale = jnp.exp(mt[tt, j] - run_m[...]) * run_s[...]
            cols = []
            for c in range(3):
                start = j * 384 + c * 128
                e = ex[tt, :, pl.ds(pl.multiple_of(start, 128), 128)] * scale
                cols.append(jnp.where(hit == tt * SHARD + start, e - 1.0, e).astype(BF16))
            return acc + dot(jnp.concatenate(cols, axis=1), eb[tt, pl.ds(pl.multiple_of(j * 384, 128), 384), :])

        acc = lax.fori_loop(0, N_SHARD * 5, back_tile, jnp.zeros((CHUNK, D), F32))
        dz_ref[...] = acc.astype(BF16)


def head1(z, tgt, table):
    return pl.pallas_call(
        head1_kernel,
        grid=(N_SHARD,),
        out_shape=(jax.ShapeDtypeStruct((CHUNK, D), BF16), jax.ShapeDtypeStruct((CHUNK, 128), F32)),
        in_specs=[pl.BlockSpec((CHUNK, D), lambda t: (0, 0)), pl.BlockSpec((CHUNK, 128), lambda t: (0, 0)),
                  pl.BlockSpec((SHARD, D), lambda t: (t, 0))],
        out_specs=(pl.BlockSpec((CHUNK, D), lambda t: (0, 0)), pl.BlockSpec((CHUNK, 128), lambda t: (0, 0))),
        scratch_shapes=[pltpu.VMEM((N_SHARD, SHARD, D), BF16), pltpu.VMEM((N_SHARD, CHUNK, SHARD), F32),
                        pltpu.VMEM((N_SHARD, 5, CHUNK, 128), F32),
                        pltpu.VMEM((CHUNK, 128), F32), pltpu.VMEM((CHUNK, 128), F32)],
        cost_estimate=pl.CostEstimate(flops=20_000_000_000, bytes_accessed=16_000_000, transcendentals=8_000_000),
        name='head_pass1',
    )(z, jnp.broadcast_to(tgt[:, None], (CHUNK, 128)), table)


P2_ROWS = 480
P2_TOK = 512


def head2_kernel(me_ref, e_ref, z_ref, lse_ref, tgt_ref, de_ref, eb):
    t = pl.program_id(0)
    base = me_ref[0] * SHARD

    @pl.when(t == 0)
    def _():
        row = lax.broadcasted_iota(jnp.int32, (SHARD, D), 0) + base
        eb[...] = jnp.where(row < VOCAB, e_ref[...], 0.0).astype(BF16)
        de_ref[...] = jnp.zeros_like(de_ref)

    z = z_ref[...]

    def part(j, carry):
        rows = pl.ds(pl.multiple_of(j * P2_ROWS, 16), P2_ROWS)
        logits = dot_nt(eb[rows, :], z)
        row = lax.broadcasted_iota(jnp.int32, (P2_ROWS, P2_TOK), 0) + (base + j * P2_ROWS)
        p = jnp.exp(logits - lse_ref[...])
        p = jnp.where(row == tgt_ref[...], p - 1.0, p).astype(BF16)
        de_ref[rows, :] += dot(p, z)
        return carry

    lax.fori_loop(0, SHARD // P2_ROWS, part, 0)

    @pl.when(t == pl.num_programs(0) - 1)
    def _():
        row = lax.broadcasted_iota(jnp.int32, (SHARD, D), 0) + base
        de_ref[...] = jnp.where(row < VOCAB, de_ref[...], 0.0)


def head2(me, table, z_all, lse, tgt):
    n_tok = z_all.shape[0]
    return pl.pallas_call(
        head2_kernel,
        grid_spec=pltpu.PrefetchScalarGridSpec(
            num_scalar_prefetch=1,
            grid=(n_tok // P2_TOK,),
            in_specs=[pl.BlockSpec((SHARD, D), lambda t, m: (m[0], 0)), pl.BlockSpec((P2_TOK, D), lambda t, m: (t, 0)),
                      pl.BlockSpec((1, P2_TOK), lambda t, m: (0, t)), pl.BlockSpec((1, P2_TOK), lambda t, m: (0, t))],
            out_specs=pl.BlockSpec((SHARD, D), lambda t, m: (0, 0)),
            scratch_shapes=[pltpu.VMEM((SHARD, D), BF16)]),
        out_shape=jax.ShapeDtypeStruct((SHARD, D), F32),
        cost_estimate=pl.CostEstimate(flops=10_000_000_000, bytes_accessed=4_000_000, transcendentals=8_000_000),
        name='head_pass2',
    )(me, table, z_all, lse.reshape(1, n_tok), tgt.reshape(1, n_tok))


def chain_kernel(st_ref, a_ref, g_ref, w1_ref, w2_ref, dl_ref, d1_ref, d2_ref):
    t = pl.program_id(0)

    @pl.when(t == 0)
    def _():
        d1_ref[...] = jnp.zeros_like(d1_ref)
        d2_ref[...] = jnp.zeros_like(d2_ref)

    def one(i, g):
        p = 3 - i
        a = a_ref[p]
        u = dot(a, w1_ref[p])
        sq = u * u
        th = jnp.tanh(u * (GELU_A + (GELU_A * GELU_B) * sq))
        cdf = 0.5 * (1.0 + th)
        slope = cdf + (0.5 * u) * (1.0 - th * th) * (GELU_A + (3.0 * GELU_A * GELU_B) * sq)
        s = (dot_nt(g, w2_ref[p]) * slope).astype(BF16)

        @pl.when(p == st_ref[0])
        def _():
            h = (u * cdf).astype(BF16)
            d2_ref[...] += dot_tn(h, g)
            d1_ref[...] += dot_tn(a, s)

        return (g.astype(F32) + dot_nt(s, w1_ref[p])).astype(BF16)

    dl_ref[...] = lax.fori_loop(0, 4, one, g_ref[...])


def chain(stage, acts, g, w1, w2):
    n = TOK // CHUNK
    return pl.pallas_call(
        chain_kernel,
        grid_spec=pltpu.PrefetchScalarGridSpec(
            num_scalar_prefetch=1,
            grid=(n,),
            in_specs=[pl.BlockSpec((4, CHUNK, D), lambda t, s: (0, t, 0)), pl.BlockSpec((CHUNK, D), lambda t, s: (t, 0)),
                      pl.BlockSpec((4, D, FF), lambda t, s: (0, 0, 0)), pl.BlockSpec((4, FF, D), lambda t, s: (0, 0, 0))],
            out_specs=(pl.BlockSpec((CHUNK, D), lambda t, s: (t, 0)), pl.BlockSpec((D, FF), lambda t, s: (0, 0)),
                       pl.BlockSpec((FF, D), lambda t, s: (0, 0)))),
        out_shape=(jax.ShapeDtypeStruct((TOK, D), BF16), jax.ShapeDtypeStruct((D, FF), F32),
                   jax.ShapeDtypeStruct((FF, D), F32)),
        cost_estimate=pl.CostEstimate(flops=5_000_000_000, bytes_accessed=4_000_000, transcendentals=2_000_000),
        name='back_chain',
    )(stage, acts, g, w1, w2)


ADD_PARTS = 16
ADD_ROWS = VOCAB // ADD_PARTS


def rows_kernel(me_ref, tok_ref, dl_ref, de_ref, g_hbm, base_hbm, sq_ref, acc, rows, in_sem, out_sem):
    n_tok = dl_ref.shape[0]
    ins = [pltpu.make_async_copy(g_hbm.at[pl.ds(k * ADD_ROWS, ADD_ROWS)], acc.at[pl.ds(k * ADD_ROWS, ADD_ROWS)], in_sem.at[k])
           for k in range(ADD_PARTS)]
    for cp in ins:
        cp.start()
    rows[...] = dl_ref[...].astype(F32) * (math.sqrt(D) / 4.0)
    for cp in ins:
        cp.wait()

    def add(i, carry):
        for j in range(8):
            r = i * 8 + j
            at = pl.ds(tok_ref[r], 1)
            acc[at, :] = acc[at, :] + rows[pl.ds(r, 1), :]
        return carry

    lax.fori_loop(0, n_tok // 8, add, 0)
    outs = [pltpu.make_async_copy(acc.at[pl.ds(k * ADD_ROWS, ADD_ROWS)], base_hbm.at[pl.ds(k * ADD_ROWS, ADD_ROWS)], out_sem.at[k])
            for k in range(ADD_PARTS)]
    for cp in outs:
        cp.start()
    base = me_ref[0] * SHARD
    row = lax.broadcasted_iota(jnp.int32, (64, D), 0)

    def square(k, total):
        at = pl.multiple_of(k * 64, 8)
        val = acc[pl.ds(pl.multiple_of(base + at, 8), 64), :] + 0.25 * de_ref[pl.ds(at, 64), :]
        val = jnp.where(row + (base + at) < VOCAB, val, 0.0)
        return total + val * val

    total = lax.fori_loop(0, SHARD // 64, square, jnp.zeros((64, D), F32))
    sq_ref[...] = jnp.full(sq_ref.shape, jnp.sum(total), F32)
    for cp in outs:
        cp.wait()


def add_rows(me, tokens, dl, de, gacc):
    return pl.pallas_call(
        rows_kernel,
        out_shape=(jax.ShapeDtypeStruct((VOCAB, D), F32), jax.ShapeDtypeStruct((8, 128), F32)),
        in_specs=[SMEM, SMEM, VMEM, VMEM, ANY],
        out_specs=(ANY, VMEM),
        scratch_shapes=[pltpu.VMEM((VPAD, D), F32), pltpu.VMEM((dl.shape[0], D), F32),
                        pltpu.SemaphoreType.DMA((ADD_PARTS,)), pltpu.SemaphoreType.DMA((ADD_PARTS,))],
        cost_estimate=pl.CostEstimate(flops=10_000_000_000, bytes_accessed=32_000_000, transcendentals=0),
        name='add_rows',
    )(me, tokens, dl, de, gacc)


def adamw_update(master, moment, velocity, gradient, clip_scale):
    g = clip_scale * gradient
    m = ADAM_BETA1 * moment + (1.0 - ADAM_BETA1) * g
    v = ADAM_BETA2 * velocity + (1.0 - ADAM_BETA2) * g * g
    m_hat = m * (1.0 / (1.0 - ADAM_BETA1 ** STEP_COUNT))
    v_hat = v * (1.0 / (1.0 - ADAM_BETA2 ** STEP_COUNT))
    w = master - LEARN_RATE * (m_hat / (jnp.sqrt(v_hat) + ADAM_EPS) + WEIGHT_DECAY * master)
    return w, m, v


def adam_kernel(c_ref, w_ref, m_ref, v_ref, b_ref, de_ref, w_out, m_out, v_out):
    w, m, v = adamw_update(w_ref[...], m_ref[...], v_ref[...], b_ref[...] + 0.25 * de_ref[...], c_ref[0])
    w_out[...] = w
    m_out[...] = m
    v_out[...] = v


def adam(c, w, m, v, base, de):
    spec = pl.BlockSpec((SHARD, D), lambda t: (t, 0))
    shape = jax.ShapeDtypeStruct((VOCAB, D), F32)
    return pl.pallas_call(
        adam_kernel,
        grid=(N_SHARD,),
        out_shape=(shape, shape, shape),
        in_specs=[SMEM] + [spec] * 5,
        out_specs=(spec, spec, spec),
        cost_estimate=pl.CostEstimate(flops=20_000_000_000, bytes_accessed=125_000_000, transcendentals=8_000_000),
        name='adam_embed',
    )(c.reshape(1), w, m, v, base, de)


FW_TOK = 512


def forward_kernel(tok_ref, table_hbm, w1_ref, w2_ref, out_ref, table, x, sem):
    t = pl.program_id(0)
    copies = [pltpu.make_async_copy(table_hbm.at[pl.ds(k * ADD_ROWS, ADD_ROWS)], table.at[pl.ds(k * ADD_ROWS, ADD_ROWS)], sem.at[k])
              for k in range(ADD_PARTS)]

    @pl.when(t == 0)
    def _():
        for cp in copies:
            cp.start()
        for cp in copies:
            cp.wait()

    def take(i, carry):
        for j in range(16):
            r = i * 16 + j
            x[pl.ds(r, 1), :] = table[pl.ds(tok_ref[t * FW_TOK + r], 1), :]
        return carry

    lax.fori_loop(0, FW_TOK // 16, take, 0)
    act = (math.sqrt(D) * x[...].astype(BF16).astype(F32)).astype(BF16)
    for p in range(4):
        act = block_forward(act, w1_ref[p], w2_ref[p])
    out_ref[...] = act


def forward(tokens, table, w1, w2):
    n = tokens.shape[0]
    return pl.pallas_call(
        forward_kernel,
        grid=(n // FW_TOK,),
        out_shape=jax.ShapeDtypeStruct((n, D), BF16),
        in_specs=[SMEM, ANY, pl.BlockSpec((4, D, FF), lambda t: (0, 0, 0)), pl.BlockSpec((4, FF, D), lambda t: (0, 0, 0))],
        out_specs=pl.BlockSpec((FW_TOK, D), lambda t: (t, 0)),
        scratch_shapes=[pltpu.VMEM((VOCAB, D), F32), pltpu.VMEM((FW_TOK, D), F32), pltpu.SemaphoreType.DMA((ADD_PARTS,))],
        name='forward',
    )(tokens, table, w1, w2)


def solution(mesh):
    w_spec = P('stage', None, None)
    in_specs = (w_spec,) * 8 + (P(None, None),) * 4 + (P('stage', 'data', None), P('data'), P('data'), P(None, 'data'), P(None))
    out_specs = (w_spec,) * 6 + (P(None, None),) * 3 + (P(None, 'data', None),)

    def local_step(w_first, w_second, mom_first, mom_second, vel_first, vel_second, grad_first, grad_second,
                   embed_table, mom_embed, vel_embed, grad_embed, stage_acts, last_tokens, targets, next_tokens, max_norm):
        stage = lax.axis_index('stage')
        data = lax.axis_index('data')
        me = (data * 4 + stage).reshape(1).astype(jnp.int32)
        w_in = w_first[0].astype(BF16)
        w_out = w_second[0].astype(BF16)
        acts = stage_acts[0]

        z_full = block_forward(acts, w_in, w_out)
        z = spread(0, z_full)
        z_all = lax.all_gather(z, ('data', 'stage'), tiled=True)
        acts_all = lax.all_gather(acts, 'stage')
        w1_all = lax.all_gather(w_in, 'stage')
        w2_all = lax.all_gather(w_out, 'stage')

        tgt = lax.dynamic_slice(targets, (stage * CHUNK,), (CHUNK,))
        dz, lse = head1(z, tgt, embed_table)
        lse_rows = lse[:, 0].reshape(2, 128)
        g, lse_all, tgt_all, tok_all = exchange(
            1, (dz, 'stage', 'gather'), (lse_rows, 'all', 'gather'),
            (targets.reshape(8, 128), 'data', 'gather'), (last_tokens.reshape(8, 128), 'data', 'gather'))
        de = head2(me, embed_table, z_all, lse_all, tgt_all)
        de_all = lax.all_gather(de, ('data', 'stage'), tiled=True)

        d_low, step_in, step_out = chain(stage.reshape(1).astype(jnp.int32), acts_all, g.reshape(TOK, D), w1_all, w2_all)
        dl_all, r1, r2 = exchange(
            2, (d_low, 'data', 'gather'), (step_in.reshape(4, D // 4, FF), 'data', 'scatter'),
            (step_out.reshape(4, FF // 4, D), 'data', 'scatter'))
        base, shard_sq = add_rows(me, tok_all.reshape(-1), dl_all.reshape(-1, D), de, grad_embed)
        part1 = lax.dynamic_slice(grad_first[0], (data * (D // 4), 0), (D // 4, FF)) + jnp.sum(r1, axis=0) * 0.25
        part2 = lax.dynamic_slice(grad_second[0], (data * (FF // 4), 0), (FF // 4, D)) + jnp.sum(r2, axis=0) * 0.25
        sq = shard_sq + (jnp.sum(part1 * part1) + jnp.sum(part2 * part2))
        sq_all, full1, full2 = exchange(3, (sq, 'all', 'gather'), (part1, 'data', 'gather'), (part2, 'data', 'gather'))
        total_sq = jnp.sum(sq_all[:, 0, 0])
        clip_scale = jnp.minimum(1.0, max_norm[0] / (jnp.sqrt(total_sq) + CLIP_EPS))

        new_first, new_mom_first, new_vel_first = adamw_update(
            w_first[0], mom_first[0], vel_first[0], full1.reshape(D, FF), clip_scale)
        new_second, new_mom_second, new_vel_second = adamw_update(
            w_second[0], mom_second[0], vel_second[0], full2.reshape(FF, D), clip_scale)
        n1_all = lax.all_gather(new_first.astype(BF16), 'stage')
        n2_all = lax.all_gather(new_second.astype(BF16), 'stage')
        new_embed, new_mom_embed, new_vel_embed = adam(clip_scale, embed_table, mom_embed, vel_embed, base, de_all)

        n_micro, tokens = next_tokens.shape
        core = lax.rem(stage, 2)
        mine = lax.dynamic_slice(next_tokens, (core * (n_micro // 2), 0), (n_micro // 2, tokens)).reshape(-1)
        half = forward(mine, new_embed, n1_all, n2_all)
        next_acts = swap(4, half).reshape(n_micro, tokens, D)
        return (new_first[None], new_second[None], new_mom_first[None], new_mom_second[None],
                new_vel_first[None], new_vel_second[None], new_embed, new_mom_embed, new_vel_embed, next_acts)

    return jax.shard_map(local_step, mesh=mesh, in_specs=in_specs, out_specs=out_specs, check_vma=False)
```
